256 devices in a mesh: tp: 32 (over z, y), dp: 8 (over x, core).
Axes of the slice: x: 4, y: 4, z: 8, core: 2. Of those that a mesh axis runs over, the one named last changes fastest.
Arguments:
- x_in: bfloat16 [16384, 896], P('dp')
- w_gate: bfloat16 [896, 4864], P('dp', 'tp')
- w_up: bfloat16 [896, 4864], P('dp', 'tp')
- w_down: bfloat16 [4864, 896], P('tp', 'dp')
- dy_in: bfloat16 [16384, 896], P('dp')
Outputs:
- output 1: bfloat16 [16384, 896], P('dp')
- output 2: bfloat16 [16384, 896], P('dp')
- output 3: float32 [896, 4864], P('dp', 'tp')
- output 4: float32 [896, 4864], P('dp', 'tp')
- output 5: float32 [4864, 896], P('tp', 'dp')
All inputs are finite; a program needn't handle non-finite values.
Results may differ from the reference program's by a relative error of at most 0.001.
Values are sent between devices in bfloat16 or wider.
A program may use at most 768 MiB of HBM per device.

```python
import jax
import jax.numpy as jnp
from jax import lax

MODEL_DIM = 896
HIDDEN_DIM = 4864
SHARD_TOKENS = 2048
DATA_SHARDS = 8


def setup_inputs(seed: int = 0) -> dict:
    key_list = jax.random.split(jax.random.key(seed), 5)
    row_count = DATA_SHARDS * SHARD_TOKENS
    x_vals = jax.random.normal(key_list[0], (row_count, MODEL_DIM), jnp.float32)
    gate_vals = jax.random.normal(key_list[1], (MODEL_DIM, HIDDEN_DIM), jnp.float32) * MODEL_DIM ** -0.5
    up_vals = jax.random.normal(key_list[2], (MODEL_DIM, HIDDEN_DIM), jnp.float32) * MODEL_DIM ** -0.5
    down_vals = jax.random.normal(key_list[3], (HIDDEN_DIM, MODEL_DIM), jnp.float32) * HIDDEN_DIM ** -0.5
    dy_vals = jax.random.normal(key_list[4], (row_count, MODEL_DIM), jnp.float32)
    return {
        'x_in': x_vals.astype(jnp.bfloat16),
        'w_gate': gate_vals.astype(jnp.bfloat16),
        'w_up': up_vals.astype(jnp.bfloat16),
        'w_down': down_vals.astype(jnp.bfloat16),
        'dy_in': dy_vals.astype(jnp.bfloat16),
    }


def reference(x_in, w_gate, w_up, w_down, dy_in):
    row_count = DATA_SHARDS * SHARD_TOKENS
    x_blocks = x_in.reshape(DATA_SHARDS, SHARD_TOKENS, MODEL_DIM)
    dy_blocks = dy_in.reshape(DATA_SHARDS, SHARD_TOKENS, MODEL_DIM)

    def shard_pass(carry, block):
        acc_gate, acc_up, acc_down = carry
        x_blk, dy_blk = block
        gate_pre = jnp.dot(x_blk, w_gate, preferred_element_type=jnp.float32)
        up_pre = jnp.dot(x_blk, w_up, preferred_element_type=jnp.float32)
        sig_gate = jax.nn.sigmoid(gate_pre)
        silu_gate = gate_pre * sig_gate
        hidden = (silu_gate * up_pre).astype(jnp.bfloat16)
        y_blk = (x_blk.astype(jnp.float32) + jnp.dot(hidden, w_down, preferred_element_type=jnp.float32)).astype(jnp.bfloat16)
        grad_h = jnp.dot(dy_blk, w_down.T, preferred_element_type=jnp.float32)
        d_gate = (grad_h * up_pre * sig_gate * (1.0 + gate_pre * (1.0 - sig_gate))).astype(jnp.bfloat16)
        d_up = (grad_h * silu_gate).astype(jnp.bfloat16)
        dx_blk = (dy_blk.astype(jnp.float32)
                  + jnp.dot(d_gate, w_gate.T, preferred_element_type=jnp.float32)
                  + jnp.dot(d_up, w_up.T, preferred_element_type=jnp.float32)).astype(jnp.bfloat16)
        acc_gate = acc_gate + jnp.dot(x_blk.T, d_gate, preferred_element_type=jnp.float32)
        acc_up = acc_up + jnp.dot(x_blk.T, d_up, preferred_element_type=jnp.float32)
        acc_down = acc_down + jnp.dot(hidden.T, dy_blk, preferred_element_type=jnp.float32)
        return (acc_gate, acc_up, acc_down), (y_blk, dx_blk)

    zero_acc = (jnp.zeros((MODEL_DIM, HIDDEN_DIM), jnp.float32),
                jnp.zeros((MODEL_DIM, HIDDEN_DIM), jnp.float32),
                jnp.zeros((HIDDEN_DIM, MODEL_DIM), jnp.float32))
    sums, outs = lax.scan(shard_pass, zero_acc, (x_blocks, dy_blocks))
    y_blocks, dx_blocks = outs
    return (y_blocks.reshape(row_count, MODEL_DIM), dx_blocks.reshape(row_count, MODEL_DIM), sums[0], sums[1], sums[2])
```

```python
import jax
import jax.numpy as jnp
from jax import lax
from jax.sharding import PartitionSpec as P

NZ, NY = 8, 4


def solution(mesh):
    z_groups = [[z * NY + y for z in range(NZ)] for y in range(NY)]
    y_groups = [[z * NY + y for y in range(NY)] for z in range(NZ)]

    def grads(x, dy, wg, wu, wd):
        f32 = jnp.float32
        a = jnp.einsum('td,fd->tf', x, wg, preferred_element_type=f32)
        b = jnp.einsum('td,fd->tf', x, wu, preferred_element_type=f32)
        g = jnp.einsum('td,fd->tf', dy, wd, preferred_element_type=f32)
        s = jax.nn.sigmoid(a)
        silu = a * s
        h = (silu * b).astype(jnp.bfloat16)
        da = (g * b * s * (1.0 + a * (1.0 - s))).astype(jnp.bfloat16)
        db = (g * silu).astype(jnp.bfloat16)
        return h, da, db

    def device_pass(x, gate, up, down, dy):
        f32 = jnp.float32
        tp = lax.axis_index('tp')
        z = tp // NY
        w = jnp.concatenate([gate.T, up.T, down], axis=0)
        w_own = lax.all_gather(w, 'dp', axis=1, tiled=True)
        w_q = lax.all_gather(w_own, 'tp', axis=0, axis_index_groups=z_groups, tiled=False)
        wg = w_q[:, 0:152].reshape(NZ * 152, 896)
        wu = w_q[:, 152:304].reshape(NZ * 152, 896)
        wd = w_q[:, 304:456].reshape(NZ * 152, 896)
        xr = lax.dynamic_slice_in_dim(x, z * 256, 256, 0)
        dyr = lax.dynamic_slice_in_dim(dy, z * 256, 256, 0)
        h, da, db = grads(xr, dyr, wg, wu, wd)
        yp = jnp.dot(h, wd, preferred_element_type=f32)
        ys = lax.psum_scatter(yp, 'tp', scatter_dimension=0, axis_index_groups=y_groups, tiled=True)
        x64 = lax.dynamic_slice_in_dim(x, tp * 64, 64, 0)
        yr = (x64.astype(f32) + ys).astype(jnp.bfloat16)
        y_out = lax.all_gather(yr, 'tp', axis=0, tiled=True)
        dxp = jnp.dot(da, wg, preferred_element_type=f32) + jnp.dot(db, wu, preferred_element_type=f32)
        dxs = lax.psum_scatter(dxp, 'tp', scatter_dimension=0, axis_index_groups=y_groups, tiled=True)
        dy64 = lax.dynamic_slice_in_dim(dy, tp * 64, 64, 0)
        dxr = (dy64.astype(f32) + dxs).astype(jnp.bfloat16)
        dx_out = lax.all_gather(dxr, 'tp', axis=0, tiled=True)
        h2, da2, db2 = grads(x, dy, w_own[0:152], w_own[152:304], w_own[304:456])
        dg = jnp.einsum('td,tf->df', x, da2, preferred_element_type=f32)
        du = jnp.einsum('td,tf->df', x, db2, preferred_element_type=f32)
        dd = jnp.einsum('td,tf->df', dy, h2, preferred_element_type=f32)
        dall = jnp.concatenate([dg, du, dd], axis=1)
        dall = lax.psum_scatter(dall, 'dp', scatter_dimension=0, tiled=True)
        return y_out, dx_out, dall[:, 0:152], dall[:, 152:304], dall[:, 304:456].T

    row_spec = P('dp', None)
    weight_spec = P('dp', 'tp')
    down_spec = P('tp', 'dp')
    return jax.shard_map(device_pass, mesh=mesh,
                         in_specs=(row_spec, weight_spec, weight_spec, down_spec, row_spec),
                         out_specs=(row_spec, row_spec, weight_spec, weight_spec, down_spec),
                         check_vma=False)
```

```python
import functools

import jax
import jax.numpy as jnp
from jax import lax
from jax.experimental import pallas as pl
from jax.experimental.pallas import tpu as pltpu
from jax.sharding import PartitionSpec as P

MESH = pl.DeviceIdType.MESH
BF16, F32 = jnp.bfloat16, jnp.float32
NX, NY = 4, 4
LANES = 128


def pad_blocks(tiles, db):
    off = LANES - db
    lane = lax.broadcasted_iota(jnp.int32, tiles[0].shape, 1)
    blocks = []
    for d in range(8):
        s = off * d
        cur = pltpu.roll(tiles[d], s, 1) if (d < 7 and s) else (tiles[d] if d < 7 else None)
        prev = pltpu.roll(tiles[d - 1], s, 1) if d else None
        if cur is None:
            b = prev
        elif prev is None:
            b = cur
        else:
            b = jnp.where(lane < s, prev, cur)
        blocks.append(jnp.where(lane < db, b, 0.0))
    return blocks


def unpad_tiles(blocks, db):
    off = LANES - db
    lane = lax.broadcasted_iota(jnp.int32, blocks[0].shape, 1)
    tiles = []
    for q in range(7):
        s = off * q
        a = pltpu.roll(blocks[q], (LANES - s) % LANES, 1) if s else blocks[q]
        b = pltpu.roll(blocks[q + 1], db - s, 1) if (db - s) % LANES else blocks[q + 1]
        tiles.append(jnp.where(lane < db - s, a, b))
    return tiles


def col_block(d):
    return (d % 2) * NX + d // 2


def nt(a, b):
    return lax.dot_general(a, b, (((1,), (1,)), ((), ())), preferred_element_type=F32)


def nn(a, b):
    return lax.dot_general(a, b, (((1,), (0,)), ((), ())), preferred_element_type=F32)


def mlp_kernel(cfg, w_ref, x_hbm, dy_hbm, y_hbm, dx_hbm, dw_ref,
               xv, dyv, xp, dyp, W, yacc, dxacc, ysend, dxsend, yrs, dxrs, yv, dxv,
               wown, dwacc, dwp, dwr1, dwr2,
               in_sem, out_sem, s_gu, s_d, s_rs, s_y, s_dx, s_dw,
               r_gz, r_gx, r_gp, r_dx4, r_dz, r_dp, r_ys, r_dxs, r_yz, r_yy, r_xy, r_xz, r_w1, r_w2):
    NZ, FP, DB = cfg["NZ"], cfg["FP"], cfg["DB"]
    T, D = xv.shape
    RZ = T // NZ
    R1 = RZ // NY
    H = NZ // 2
    KP = 8 * LANES

    t = lax.axis_index("tp")
    d = lax.axis_index("dp")
    z, y = lax.div(t, NY), lax.rem(t, NY)
    x, c = lax.div(d, 2), lax.rem(d, 2)

    def wrap(v, n):
        return lax.rem(v + n, n)

    def dev(dz=0, dy_=0, dx_=0, core=None):
        tp = wrap(z + dz, NZ) * NY + wrap(y + dy_, NY)
        dp = wrap(x + dx_, NX) * 2 + (c if core is None else core)
        return {"tp": tp, "dp": dp}

    partner = dev(core=1 - c)

    def mo(v, m):
        return pl.multiple_of(v, m)

    def remote(src, dst, ssem, rsem, to):
        return pltpu.make_async_remote_copy(src_ref=src, dst_ref=dst, send_sem=ssem, recv_sem=rsem,
                                            device_id=to, device_id_type=MESH)

    def arrived(dst, rsem):
        remote(dst, dst, s_gu.at[0], rsem, partner).wait_recv()

    def zs_of(m):
        if m == 0:
            return z
        k = (m + 1) // 2
        return wrap(z - k, NZ) if m % 2 else wrap(z + k, NZ)

    def rows_w(zs):
        return pl.ds(mo(zs * FP, FP), FP)

    def half_w(cc):
        return pl.ds(mo(cc * (NX * LANES), NX * LANES), NX * LANES)

    def blk_w(xs, cc):
        return pl.ds(mo((cc * NX + xs) * LANES, LANES), LANES)

    def gu(zs, xs):
        return W.at[0:2, rows_w(zs), blk_w(xs, c)]

    def gu_half(zs, xs, h):
        return W.at[h, rows_w(zs), blk_w(xs, c)]

    def gu_all(zs, cc):
        return W.at[0:2, rows_w(zs), half_w(cc)]

    def dn(zs, xs):
        return W.at[2, rows_w(zs), blk_w(xs, c)]

    def dn_all(zs, cc):
        return W.at[2, rows_w(zs), half_w(cc)]

    def dn_half(zs, h):
        w2 = NX * LANES // 2
        return W.at[2, rows_w(zs), pl.ds(mo(c * (NX * LANES) + h * w2, w2), w2)]

    def rows(buf, zs, ys):
        return buf.at[pl.ds(mo((zs * NY + ys) * R1, R1), R1)]

    def rows_half(buf, zs, ys, h):
        return buf.at[pl.ds(mo((zs * NY + ys) * R1 + h * (R1 // 2), R1 // 2), R1 // 2)]

    def rows_z(buf, zs):
        return buf.at[pl.ds(mo(zs * RZ, RZ), RZ)]

    barrier = pltpu.get_barrier_semaphore()
    peers = [dev(dz=1), dev(dz=-1), dev(dy_=1), dev(dy_=-1), dev(dy_=2), dev(dx_=1), dev(dx_=-1), dev(dx_=2), partner]
    for p in peers:
        pl.semaphore_signal(barrier, inc=1, device_id=p, device_id_type=MESH)

    ld_x = pltpu.make_async_copy(x_hbm, xv, in_sem.at[0])
    ld_dy = pltpu.make_async_copy(dy_hbm, dyv, in_sem.at[1])
    ld_x.start()
    ld_dy.start()
    W[:, rows_w(z), blk_w(x, c)] = w_ref[...]
    pl.semaphore_wait(barrier, len(peers))

    def send_d_own():
        for i, dx_ in enumerate((1, -1, 2)):
            remote(w_ref.at[2], dn(z, x), s_d.at[0], r_dx4.at[i], dev(dx_=dx_)).start()

    def wait_d_own():
        for i, dx_ in enumerate((-1, 1, 2)):
            arrived(dn(z, wrap(x + dx_, NX)), r_dx4.at[i])

    def send_d_z(k):
        zm, zp = wrap(z - k, NZ), wrap(z + k, NZ)
        if k < H - 1:
            remote(dn_all(zm, c), dn_all(zm, c), s_d.at[1], r_dz.at[0, k], dev(dz=1)).start()
            remote(dn_all(zp, c), dn_all(zp, c), s_d.at[1], r_dz.at[1, k], dev(dz=-1)).start()
        elif k == H - 1:
            remote(dn_half(zm, 0), dn_half(zm, 0), s_d.at[1], r_dz.at[0, k], dev(dz=1)).start()
            remote(dn_half(zp, 1), dn_half(zp, 1), s_d.at[1], r_dz.at[1, k], dev(dz=-1)).start()

    def wait_d_z(k):
        zm, zp = wrap(z - k, NZ), wrap(z + k, NZ)
        if k < H:
            arrived(dn_all(zm, c), r_dz.at[0, k - 1])
            arrived(dn_all(zp, c), r_dz.at[1, k - 1])
        else:
            arrived(dn_half(zm, 0), r_dz.at[0, k - 1])
            arrived(dn_half(zp, 1), r_dz.at[1, k - 1])

    def send_d_p(m):
        zs = zs_of(m)
        remote(dn_all(zs, c), dn_all(zs, c), s_d.at[2], r_dp.at[m], partner).start()

    def send_g_z(k):
        zm, zp = wrap(z - k, NZ), wrap(z + k, NZ)
        if k < H - 1:
            sm = w_ref.at[0:2] if k == 0 else gu(zm, x)
            sp = w_ref.at[0:2] if k == 0 else gu(zp, x)
            remote(sm, gu(zm, x), s_gu.at[0], r_gz.at[0, k], dev(dz=1)).start()
            remote(sp, gu(zp, x), s_gu.at[0], r_gz.at[1, k], dev(dz=-1)).start()
        elif k == H - 1:
            remote(gu_half(zm, x, 0), gu_half(zm, x, 0), s_gu.at[0], r_gz.at[0, k], dev(dz=1)).start()
            remote(gu_half(zp, x, 1), gu_half(zp, x, 1), s_gu.at[0], r_gz.at[1, k], dev(dz=-1)).start()

    def wait_g_z(k):
        zm, zp = wrap(z - k, NZ), wrap(z + k, NZ)
        if k < H:
            arrived(gu(zm, x), r_gz.at[0, k - 1])
            arrived(gu(zp, x), r_gz.at[1, k - 1])
        else:
            arrived(gu_half(zm, x, 0), r_gz.at[0, k - 1])
            arrived(gu_half(zp, x, 1), r_gz.at[1, k - 1])

    def send_g_x(m):
        zs = zs_of(m)
        src = w_ref.at[0:2] if m == 0 else gu(zs, x)
        remote(src, gu(zs, x), s_gu.at[1], r_gx.at[0, m], dev(dx_=1)).start()
        remote(src, gu(zs, x), s_gu.at[1], r_gx.at[1, m], dev(dx_=-1)).start()

    def fwd_g_x(m):
        zs = zs_of(m)
        xm, xq = wrap(x - 1, NX), wrap(x + 1, NX)
        arrived(gu(zs, xm), r_gx.at[0, m])
        if m % 2 == 0:
            remote(gu(zs, xm), gu(zs, xm), s_gu.at[1], r_gx.at[2, m], dev(dx_=1)).start()
        arrived(gu(zs, xq), r_gx.at[1, m])
        if m % 2 == 1:
            remote(gu(zs, xq), gu(zs, xq), s_gu.at[1], r_gx.at[2, m], dev(dx_=-1)).start()

    def send_g_p(m):
        zs = zs_of(m)
        arrived(gu(zs, wrap(x + 2, NX)), r_gx.at[2, m])
        remote(gu_all(zs, c), gu_all(zs, c), s_gu.at[2], r_gp.at[m], partner).start()

    def wait_p(m):
        zs = zs_of(m)
        arrived(gu_all(zs, 1 - c), r_gp.at[m])
        arrived(dn_all(zs, 1 - c), r_dp.at[m])

    def pad_rows(src, dst):
        def body(i, _):
            r = pl.ds(mo(i * 32, 32), 32)
            rs = pl.ds(mo(z * RZ + i * 32, 32), 32)
            v = src[rs, :].astype(F32)
            blocks = pad_blocks([v[:, q * LANES:(q + 1) * LANES] for q in range(7)], DB)
            for dd in range(8):
                j = col_block(dd)
                dst[r, j * LANES:(j + 1) * LANES] = blocks[dd].astype(BF16)
            return 0
        lax.fori_loop(0, RZ // 32, body, 0)

    def act(a, b, g):
        s = jax.nn.sigmoid(a)
        silu = a * s
        h = (silu * b).astype(BF16)
        da = (g * b * s * (1.0 + a * (1.0 - s))).astype(BF16)
        db = (g * silu).astype(BF16)
        return h, da, db

    def slice_acts(m):
        r = rows_w(zs_of(m))
        a = nt(xp[...], W[0, r, :])
        b = nt(xp[...], W[1, r, :])
        g = nt(dyp[...], W[2, r, :])
        return act(a, b, g)

    def slice_y(m, h):
        r = rows_w(zs_of(m))
        p = nn(h, W[2, r, :])
        yacc[...] = p if m == 0 else yacc[...] + p

    def slice_dx(m, da, db):
        r = rows_w(zs_of(m))
        p = nn(da, W[0, r, :]) + nn(db, W[1, r, :])
        dxacc[...] = p if m == 0 else dxacc[...] + p

    def compute(m):
        h, da, db = slice_acts(m)
        slice_y(m, h)
        slice_dx(m, da, db)

    def unpad_rows(src, dst):
        def body(i, _):
            r = pl.ds(mo(i * 32, 32), 32)
            blocks = [src[r, col_block(dd) * LANES:(col_block(dd) + 1) * LANES] for dd in range(8)]
            for q, tile in enumerate(unpad_tiles(blocks, DB)):
                dst[r, q * LANES:(q + 1) * LANES] = tile
            return 0
        lax.fori_loop(0, RZ // 32, body, 0)

    def part(buf, ys):
        return buf.at[pl.ds(mo(ys * R1, R1), R1)]

    def send_rs(buf, rbuf, ssem, rsem):
        for i, dy_ in enumerate((1, -1, 2)):
            remote(part(buf, wrap(y + dy_, NY)), rbuf.at[i], ssem, rsem.at[i], dev(dy_=dy_)).start()

    def finish_rs(buf, rbuf, rsem, base, out):
        for i in range(3):
            arrived(rbuf.at[i], rsem.at[i])
        own = pl.ds(mo(y * R1, R1), R1)
        g = pl.ds(mo(t * R1, R1), R1)
        s = buf[own, :] + rbuf[0] + rbuf[1] + rbuf[2]
        out[g, :] = (base[g, :].astype(F32) + s).astype(BF16)

    def send_y_z(k):
        zm, zp = wrap(z - k, NZ), wrap(z + k, NZ)
        if k < H - 1:
            remote(rows(yv, zm, y), rows(yv, zm, y), s_y.at[0], r_yz.at[0, k], dev(dz=1)).start()
            remote(rows(yv, zp, y), rows(yv, zp, y), s_y.at[0], r_yz.at[1, k], dev(dz=-1)).start()
        elif k == H - 1:
            remote(rows_half(yv, zm, y, 0), rows_half(yv, zm, y, 0), s_y.at[0], r_yz.at[0, k], dev(dz=1)).start()
            remote(rows_half(yv, zp, y, 1), rows_half(yv, zp, y, 1), s_y.at[0], r_yz.at[1, k], dev(dz=-1)).start()

    def wait_y_z(k):
        zm, zp = wrap(z - k, NZ), wrap(z + k, NZ)
        if k < H:
            arrived(rows(yv, zm, y), r_yz.at[0, k - 1])
            arrived(rows(yv, zp, y), r_yz.at[1, k - 1])
        else:
            arrived(rows_half(yv, zm, y, 0), r_yz.at[0, k - 1])
            arrived(rows_half(yv, zp, y, 1), r_yz.at[1, k - 1])

    def send_y_y(m):
        b = rows(yv, zs_of(m), y)
        remote(b, b, s_y.at[1], r_yy.at[0, m], dev(dy_=1)).start()
        remote(b, b, s_y.at[1], r_yy.at[1, m], dev(dy_=-1)).start()

    def fwd_y_y(m):
        zs = zs_of(m)
        bm, bq = rows(yv, zs, wrap(y - 1, NY)), rows(yv, zs, wrap(y + 1, NY))
        arrived(bm, r_yy.at[0, m])
        if m % 2 == 0:
            remote(bm, bm, s_y.at[1], r_yy.at[2, m], dev(dy_=1)).start()
        arrived(bq, r_yy.at[1, m])
        if m % 2 == 1:
            remote(bq, bq, s_y.at[1], r_yy.at[2, m], dev(dy_=-1)).start()

    def end_y_y(m):
        zs = zs_of(m)
        arrived(rows(yv, zs, wrap(y + 2, NY)), r_yy.at[2, m])
        pltpu.make_async_copy(rows_z(yv, zs), rows_z(y_hbm, zs), out_sem.at[0, m]).start()

    SUB = (0, -1, 1, 2)

    def send_x_y():
        b = rows(dxv, z, y)
        for i, dy_ in enumerate((1, -1, 2)):
            remote(b, b, s_dx.at[0], r_xy.at[i], dev(dy_=dy_)).start()

    def wait_x_y(i):
        dy_ = (-1, 1, 2)[i]
        arrived(rows(dxv, z, wrap(y + dy_, NY)), r_xy.at[i])

    def send_x_z(k, s):
        zm, zp = wrap(z - k, NZ), wrap(z + k, NZ)
        ys = wrap(y + SUB[s], NY)
        if k < H - 1 or (k == H - 1 and s % 2 == 0):
            remote(rows(dxv, zm, ys), rows(dxv, zm, ys), s_dx.at[1], r_xz.at[0, k, s], dev(dz=1)).start()
        if k < H - 1 or (k == H - 1 and s % 2 == 1):
            remote(rows(dxv, zp, ys), rows(dxv, zp, ys), s_dx.at[1], r_xz.at[1, k, s], dev(dz=-1)).start()

    def wait_x_z(k, s):
        zm, zp = wrap(z - k, NZ), wrap(z + k, NZ)
        ys = wrap(y + SUB[s], NY)
        if k < H or s % 2 == 0:
            arrived(rows(dxv, zm, ys), r_xz.at[0, k - 1, s])
        if k < H or s % 2 == 1:
            arrived(rows(dxv, zp, ys), r_xz.at[1, k - 1, s])

    def out_x(m):
        zs = zs_of(m)
        pltpu.make_async_copy(rows_z(dxv, zs), rows_z(dx_hbm, zs), out_sem.at[1, m]).start()

    CH = cfg["CH"]
    n_chunks = T // CH

    def own_weights():
        def body(i, _):
            kind, r0 = lax.div(i, FP // 32), lax.rem(i, FP // 32)
            r = pl.ds(mo(z * FP + r0 * 32, 32), 32)
            v = W[kind, r, :].astype(F32)
            blocks = [v[:, col_block(dd) * LANES:(col_block(dd) + 1) * LANES] for dd in range(8)]
            o = pl.ds(mo(i * 32, 32), 32)
            for q, tile in enumerate(unpad_tiles(blocks, DB)):
                wown[o, q * LANES:(q + 1) * LANES] = tile.astype(BF16)
            return 0
        lax.fori_loop(0, 3 * FP // 32, body, 0)

    def dw_chunk(i):
        r = pl.ds(i * CH, CH)
        xb, dyb = xv[r, :], dyv[r, :]
        ab = nt(wown[0:2 * FP, :], xb)
        g = nt(wown[2 * FP:3 * FP, :], dyb)
        h, da, db = act(ab[0:FP], ab[FP:2 * FP], g)
        for q, (lhs, rhs) in enumerate(((da, xb), (db, xb), (h, dyb))):
            o = pl.ds(q * FP, FP)
            p = nn(lhs, rhs)
            dwacc[o, :] = p if i == 0 else dwacc[o, :] + p

    def dw_blocks():
        def body(i, _):
            r = pl.ds(mo(i * 32, 32), 32)
            v = dwacc[r, :]
            blocks = pad_blocks([v[:, q * LANES:(q + 1) * LANES] for q in range(7)], DB)
            for dd in range(8):
                dwp[col_block(dd), r, :] = blocks[dd]
            return 0
        lax.fori_loop(0, 3 * FP // 32, body, 0)

    def send_w1():
        src = dwp.at[pl.ds((1 - c) * NX, NX)]
        remote(src, dwr1, s_dw.at[0], r_w1.at[0], partner).start()

    def send_w2():
        arrived(dwr1, r_w1.at[0])
        for dx_ in (1, -1, 2, 0):
            xs = wrap(x + dx_, NX)
            dwp[c * NX + xs] = dwp[c * NX + xs] + dwr1[xs]
        for i, dx_ in enumerate((1, -1, 2)):
            xs = wrap(x + dx_, NX)
            remote(dwp.at[c * NX + xs], dwr2.at[i], s_dw.at[1], r_w2.at[i], dev(dx_=dx_)).start()

    def finish_w():
        for i in range(3):
            arrived(dwr2.at[i], r_w2.at[i])
        dw_ref[...] = dwp[c * NX + x] + dwr2[0] + dwr2[1] + dwr2[2]

    def ms(k):
        if k == 0:
            return (0,)
        return (2 * k - 1, 2 * k) if k < H else (NZ - 1,)

    send_g_z(0)
    send_d_own()
    send_g_x(0)
    ld_x.wait()
    pad_rows(xv, xp)
    wait_d_own()
    send_d_z(0)
    send_d_p(0)
    ld_dy.wait()
    pad_rows(dyv, dyp)

    last = NZ - 1
    acts = None
    for k in range(1, H + 3):
        if k <= H:
            wait_g_z(k)
            send_g_z(k)
            for m in ms(k):
                send_g_x(m)
        if k - 1 <= H:
            for m in ms(k - 1):
                fwd_g_x(m)
            if k >= 2:
                wait_d_z(k - 1)
                send_d_z(k - 1)
                for m in ms(k - 1):
                    send_d_p(m)
            for m in ms(k - 1):
                send_g_p(m)
        if k - 2 >= 0 and k - 2 < H:
            for m in ms(k - 2):
                wait_p(m)
                compute(m)
    wait_p(last)
    h, da, db = slice_acts(last)
    slice_y(last, h)
    unpad_rows(yacc, ysend)
    send_rs(ysend, yrs, s_rs.at[0], r_ys)
    slice_dx(last, da, db)
    unpad_rows(dxacc, dxsend)
    send_rs(dxsend, dxrs, s_rs.at[1], r_dxs)
    own_weights()
    finish_rs(ysend, yrs, r_ys, xv, yv)
    send_y_z(0)
    send_y_y(0)
    dw_chunk(0)
    wait_y_z(1)
    send_y_z(1)
    finish_rs(dxsend, dxrs, r_dxs, dyv, dxv)
    send_x_z(0, 0)
    send_x_y()
    for m in ms(1):
        send_y_y(m)
    nxt = 1

    def more():
        nonlocal nxt
        if nxt < n_chunks:
            dw_chunk(nxt)
            nxt += 1
            if nxt == n_chunks:
                dw_blocks()
                send_w1()

    for k in range(2, H + 1):
        more()
        wait_y_z(k)
        send_y_z(k)
        if k == 2:
            for i in range(3):
                wait_x_y(i)
                send_x_z(0, i + 1)
        for m in ms(k):
            send_y_y(m)
        for m in ms(k - 2):
            fwd_y_y(m)
        more()
        for s in range(4):
            wait_x_z(k - 1, s)
            send_x_z(k - 1, s)
        out_x(0) if k == 2 else [out_x(m) for m in ms(k - 2)]
    while nxt < n_chunks:
        more()
    for m in ms(H - 1):
        fwd_y_y(m)
    for m in ms(H):
        fwd_y_y(m)
    send_w2()
    for m in ms(H - 1):
        out_x(m)
    for m in range(NZ):
        end_y_y(m)
    for s in range(4):
        wait_x_z(H, s)
    out_x(last)
    finish_w()

    def sent(total, sem):
        remote(total, total, sem, r_w1.at[0], partner).wait_send()

    n1 = NZ - 1
    sent(W.at[0:2, 0:n1 * FP, 0:LANES], s_gu.at[0])
    sent(W.at[0:2, :, 0:3 * LANES], s_gu.at[1])
    sent(W.at[0:2, :, 0:NX * LANES], s_gu.at[2])
    sent(W.at[2, 0:FP, 0:3 * LANES], s_d.at[0])
    sent(W.at[2, 0:n1 * FP, 0:NX * LANES], s_d.at[1])
    sent(W.at[2, :, 0:NX * LANES], s_d.at[2])
    sent(yrs, s_rs.at[0])
    sent(dxrs, s_rs.at[1])
    sent(yv.at[0:n1 * R1], s_y.at[0])
    sent(yv.at[0:3 * NZ * R1], s_y.at[1])
    sent(dxv.at[0:3 * R1], s_dx.at[0])
    sent(dxv.at[0:4 * n1 * R1], s_dx.at[1])
    sent(dwr1, s_dw.at[0])
    sent(dwr2, s_dw.at[1])
    for m in range(NZ):
        zs = zs_of(m)
        pltpu.make_async_copy(rows_z(yv, zs), rows_z(y_hbm, zs), out_sem.at[0, m]).wait()
        pltpu.make_async_copy(rows_z(dxv, zs), rows_z(dx_hbm, zs), out_sem.at[1, m]).wait()


def mlp_call(cfg, w, x, dy):
    NZ, FP = cfg["NZ"], cfg["FP"]
    T, D = x.shape
    RZ = T // NZ
    R1 = RZ // NY
    H = NZ // 2
    KP = 8 * LANES
    dma = pltpu.SemaphoreType.DMA
    vm = pltpu.VMEM
    return pl.pallas_call(
        functools.partial(mlp_kernel, cfg),
        name="mlp",
        out_shape=(jax.ShapeDtypeStruct((T, D), BF16), jax.ShapeDtypeStruct((T, D), BF16),
                   jax.ShapeDtypeStruct((3 * FP, LANES), F32)),
        in_specs=[pl.BlockSpec(memory_space=pltpu.VMEM), pl.BlockSpec(memory_space=pl.ANY), pl.BlockSpec(memory_space=pl.ANY)],
        out_specs=(pl.BlockSpec(memory_space=pl.ANY), pl.BlockSpec(memory_space=pl.ANY), pl.BlockSpec(memory_space=pltpu.VMEM)),
        scratch_shapes=[
            vm((T, D), BF16), vm((T, D), BF16), vm((RZ, KP), BF16), vm((RZ, KP), BF16), vm((3, NZ * FP, KP), BF16),
            vm((RZ, KP), F32), vm((RZ, KP), F32), vm((RZ, D), F32), vm((RZ, D), F32),
            vm((3, R1, D), F32), vm((3, R1, D), F32), vm((T, D), BF16), vm((T, D), BF16),
            vm((3 * FP, D), BF16), vm((3 * FP, D), F32), vm((8, 3 * FP, LANES), F32),
            vm((NX, 3 * FP, LANES), F32), vm((3, 3 * FP, LANES), F32),
            dma((2,)), dma((2, NZ)), dma((3,)), dma((3,)), dma((2,)), dma((2,)), dma((2,)), dma((2,)),
            dma((2, H)), dma((3, NZ)), dma((NZ,)), dma((3,)), dma((2, H)), dma((NZ,)), dma((3,)), dma((3,)),
            dma((2, H)), dma((3, NZ)), dma((3,)), dma((2, H, 4)), dma((1,)), dma((3,)),
        ],
        compiler_params=pltpu.CompilerParams(collective_id=0, has_side_effects=True, vmem_limit_bytes=60 * 1024 * 1024),
    )(w, x, dy)


def solution(mesh):
    nz = mesh.shape["tp"] // NY

    def device_pass(x, gate, up, down, dy):
        db, f = gate.shape
        fp = -(-f // 32) * 32
        cfg = {"NZ": nz, "FP": fp, "DB": db, "CH": min(256, x.shape[0])}
        pad = lambda a: jnp.pad(a, ((0, fp - f), (0, LANES - db)))
        w = jnp.stack([pad(gate.T), pad(up.T), pad(down)])
        y, dx, dw = mlp_call(cfg, w, x, dy)
        dw = dw.reshape(3, fp, LANES)[:, :f, :db]
        return y, dx, dw[0].T, dw[1].T, dw[2]

    row, col, low = P("dp", None), P("dp", "tp"), P("tp", "dp")
    return jax.shard_map(device_pass, mesh=mesh, in_specs=(row, col, col, low, row),
                         out_specs=(row, row, col, col, low), check_vma=False)
```
